32 devices in a mesh: grp: 4 (over x, core), mem: 8 (over z, y).
Axes of the slice: x: 2, y: 2, z: 4, core: 2. Of those that a mesh axis runs over, the one named last changes fastest.
Arguments:
- source_pts: float32 [64, 8192], P(None, ('grp', 'mem')), may hold values from -30 to 30
- target_pts: float32 [64, 8192], P(None, ('grp', 'mem')), may hold values from -30 to 30
- source_pot: float32 [8192], P(('grp', 'mem')), may hold values from -8 to 520
- target_pot: float32 [8192], P(('grp', 'mem')), may hold values from -8 to 520
- source_logw: float32 [8192], P(('grp', 'mem')), may hold values from -1 to 4
- target_logw: float32 [8192], P(('grp', 'mem')), may hold values from -1 to 4
Outputs:
- source_new: float32 [8192], P(('grp', 'mem'))
- target_new: float32 [8192], P(('grp', 'mem'))
The draws below stay inside these ranges and needn't reach their ends.
All inputs are finite; a program needn't handle non-finite values.
Results may differ from the reference program's by a relative error of at most 0.0001.
Values sent between devices are 32-bit elements; how exact they have to be, the bound alone decides.
A program may use at most 64 MiB of HBM per device.

```python
import math
import jax
import jax.numpy as jnp
from jax import lax

FEAT = 64
POINTS = 8192


def cloud_draw(key, salt):
    first = jax.random.fold_in(key, salt)
    base = jnp.clip(jax.random.normal(first, (FEAT, POINTS), jnp.float32), -6.0, 6.0)
    return base


def potential_draw(key, salt):
    first = jax.random.fold_in(key, salt)
    base = jax.random.uniform(first, (POINTS,), jnp.float32, -8.0, 8.0)
    return base


def weight_draw(key, salt):
    first = jax.random.fold_in(key, salt)
    ramp = jnp.arange(POINTS).astype(jnp.float32) / POINTS
    noise = jax.random.uniform(first, (POINTS,), jnp.float32, -1.0, 1.0)
    return noise + jnp.log1p(2.0 * ramp)


def draw_source_pts(key, part):
    return cloud_draw(key, 11)


def draw_target_pts(key, part):
    return cloud_draw(key, 23)


def draw_source_pot(key, part):
    return potential_draw(key, 37)


def draw_target_pot(key, part):
    return potential_draw(key, 41)


def draw_source_logw(key, part):
    return weight_draw(key, 53)


def draw_target_logw(key, part):
    return weight_draw(key, 67)


def setup_inputs(seed: int = 0) -> dict:
    streams_of = jax.random.split(jax.random.key(seed), 7)
    source_pts = draw_source_pts(jax.random.fold_in(streams_of[6], 71), 0)
    target_pts = draw_target_pts(jax.random.fold_in(streams_of[6], 71), 0)
    source_pot = draw_source_pot(jax.random.fold_in(streams_of[6], 71), 0)
    target_pot = draw_target_pot(jax.random.fold_in(streams_of[6], 71), 0)
    source_logw = draw_source_logw(jax.random.fold_in(streams_of[6], 71), 0)
    target_logw = draw_target_logw(jax.random.fold_in(streams_of[6], 71), 0)
    return dict(source_pts=source_pts, target_pts=target_pts, source_pot=source_pot, target_pot=target_pot, source_logw=source_logw, target_logw=target_logw)


epsilon = 4.0
floor_value = -1e30


def log_total(values):
    peak = jnp.max(values)
    return peak + jnp.log(jnp.sum(jnp.exp(values - peak)))


def reference(source_pts, target_pts, source_pot, target_pot, source_logw, target_logw):
    src_log = source_logw - log_total(source_logw)
    tgt_log = target_logw - log_total(target_logw)
    src_sq = 0.5 * jnp.sum(source_pts * source_pts, 0)
    tgt_sq = 0.5 * jnp.sum(target_pts * target_pts, 0)
    row_term = src_log + source_pot / epsilon
    col_term = tgt_log + target_pot / epsilon
    width = math.gcd(POINTS, 512)
    count = POINTS // width
    xs = source_pts.reshape(FEAT, count, width).transpose(1, 0, 2)
    terms = row_term.reshape(count, width)
    squares = src_sq.reshape(count, width)

    def step(carry, item):
        col_max, col_sum = carry
        xblock, rblock, qblock = item
        cross = lax.dot_general(xblock, target_pts, (((0,), (0,)), ((), ())),
                                precision=lax.Precision.HIGHEST, preferred_element_type=jnp.float32)
        half = (qblock[:, None] + tgt_sq[None, :] - cross) / epsilon
        scores = col_term[None, :] - half
        peak = jnp.max(scores, 1)
        row_hat = -epsilon * (peak + jnp.log(jnp.sum(jnp.exp(scores - peak[:, None]), 1)))
        others = rblock[:, None] - half
        bmax = jnp.maximum(col_max, jnp.max(others, 0))
        col_sum = col_sum * jnp.exp(col_max - bmax) + jnp.sum(jnp.exp(others - bmax[None, :]), 0)
        return (bmax, col_sum), row_hat

    init = (jnp.full((POINTS,), floor_value, jnp.float32), jnp.zeros((POINTS,), jnp.float32))
    (col_max, col_sum), row_hat = lax.scan(step, init, (xs, terms, squares))
    col_hat = -epsilon * (col_max + jnp.log(col_sum))
    source_new = 0.5 * (source_pot + row_hat.reshape(POINTS))
    target_new = 0.5 * (target_pot + col_hat)
    return source_new, target_new
```

```python
import functools
import math

import jax
import jax.numpy as jnp
from jax import lax
from jax.experimental import pallas as pl
from jax.experimental.pallas import tpu as pltpu
from jax.sharding import PartitionSpec as P

MESH = pl.DeviceIdType.MESH
epsilon = 4.0
log2e = math.log2(math.e)
ln2 = math.log(2.0)


def inner_size(groups, members):
    inner = 1
    while members % inner or groups * inner < members // inner:
        inner += 1
    return inner


def split3(v):
    hi = v.astype(jnp.bfloat16)
    rest = v - hi.astype(jnp.float32)
    mid = rest.astype(jnp.bfloat16)
    low = (rest - mid.astype(jnp.float32)).astype(jnp.bfloat16)
    return hi, mid, low


def term_of(points, pot, logw):
    half = 0.5 * jnp.sum(points * points, 0, keepdims=True)
    return (logw + (pot - half) / epsilon) * log2e


def extra_rows(term, first):
    width = term.shape[1]
    hi, mid, low = (v.astype(jnp.float32) for v in split3(term))
    line = lax.broadcasted_iota(jnp.int32, (16, width), 0)
    base = 0 if first else 3
    ones = 3 - base
    out = jnp.where((line >= ones) & (line < ones + 3), 1.0, 0.0)
    for k, part in enumerate((hi, mid, low)):
        out = jnp.where(line == base + k, part, out)
    return out.astype(jnp.bfloat16)


def pack_left(points, pot, logw):
    hi, mid, low = split3(points * (log2e / epsilon))
    return jnp.concatenate(
        [hi, hi, mid, mid, hi, low, extra_rows(term_of(points, pot, logw), True)], 0
    )


def pack_right(points, pot, logw):
    hi, mid, low = split3(points)
    return jnp.concatenate(
        [hi, mid, hi, mid, low, hi, extra_rows(term_of(points, pot, logw), False)], 0
    )


def kernel(
    groups,
    inner,
    outer,
    x_ref,
    y_ref,
    xpot_ref,
    ypot_ref,
    xlog_ref,
    ylog_ref,
    xout_ref,
    yout_ref,
    xbuf,
    xpot,
    xlog,
    ybuf,
    ypot,
    ylog,
    ypack,
    cmax,
    csum,
    rowmsg,
    rowres,
    colmsg,
    colres,
    local_sem,
    xsend,
    xrecv,
    ysend,
    yrecv,
    rsend,
    rrecv,
    csend,
    crecv,
):
    plane = groups * inner
    rows = xbuf.shape[2]
    g = lax.axis_index("grp")
    mem = lax.axis_index("mem")
    z = mem // inner
    i = mem % inner
    me = g * inner + i

    def plane_dev(p):
        return (p // inner, z * inner + p % inner)

    def outer_dev(q):
        return (g, q * inner + i)

    xs = ((x_ref, xbuf), (xpot_ref, xpot), (xlog_ref, xlog))
    ys = ((y_ref, ybuf), (ypot_ref, ypot), (ylog_ref, ylog))
    locals_ = [
        pltpu.make_async_copy(src, dst.at[slot], local_sem.at[k])
        for k, (src, dst, slot) in enumerate(
            [(s, d, z) for s, d in ys] + [(s, d, me) for s, d in xs]
        )
    ]
    for c in locals_:
        c.start()

    barrier = pltpu.get_barrier_semaphore()
    for t in range(1, plane):
        pl.semaphore_signal(
            barrier, inc=1, device_id=plane_dev((me + t) % plane), device_id_type=MESH
        )
    for t in range(1, outer):
        pl.semaphore_signal(
            barrier, inc=1, device_id=outer_dev((z + t) % outer), device_id_type=MESH
        )
    for c in locals_:
        c.wait()
    pl.semaphore_wait(barrier, plane + outer - 2)

    def xcopy(k, slot, dest):
        dst = xs[k][1]
        return pltpu.make_async_remote_copy(
            src_ref=dst.at[slot],
            dst_ref=dst.at[slot],
            send_sem=xsend.at[k, dest],
            recv_sem=xrecv.at[k, slot],
            device_id=plane_dev(dest),
            device_id_type=MESH,
        )

    def ycopy(k, slot, dest):
        dst = ys[k][1]
        return pltpu.make_async_remote_copy(
            src_ref=dst.at[slot],
            dst_ref=dst.at[slot],
            send_sem=ysend.at[k, dest],
            recv_sem=yrecv.at[k, slot],
            device_id=outer_dev(dest),
            device_id_type=MESH,
        )

    def rowcopy(slot, dest):
        return pltpu.make_async_remote_copy(
            src_ref=rowmsg.at[dest],
            dst_ref=rowres.at[slot],
            send_sem=rsend.at[dest],
            recv_sem=rrecv.at[slot],
            device_id=plane_dev(dest),
            device_id_type=MESH,
        )

    def colcopy(slot, dest):
        return pltpu.make_async_remote_copy(
            src_ref=colmsg.at[dest],
            dst_ref=colres.at[slot],
            send_sem=csend.at[dest],
            recv_sem=crecv.at[slot],
            device_id=outer_dev(dest),
            device_id_type=MESH,
        )

    for t in range(1, outer):
        for k in range(3):
            ycopy(k, z, (z + t) % outer).start()
    for t in range(1, plane):
        for k in range(3):
            xcopy(k, me, (me + plane - t) % plane).start()

    def right_block(q):
        at = pl.ds(pl.multiple_of(q * rows, rows), rows)
        ypack[:, at] = pack_right(ybuf[q], ypot[q], ylog[q])

    right_block(z)
    for t in range(1, outer):
        q = (z + outer - t) % outer
        for k in range(3):
            ycopy(k, q, q).wait_recv()
        right_block(q)

    cmax[...] = jnp.full(cmax.shape, -3e38, jnp.float32)
    csum[...] = jnp.zeros(csum.shape, jnp.float32)
    tlog = jnp.concatenate([ylog[q] for q in range(outer)], 1)
    tpeak = jnp.max(tlog)
    tmass = jnp.sum(jnp.exp(tlog - tpeak))
    lane = lax.broadcasted_iota(jnp.int32, (rows, 128), 1)

    def step(t, _):
        p = (me + t) % plane

        @pl.when(t > 0)
        def _():
            for k in range(3):
                xcopy(k, p, p).wait_recv()

        left = pack_left(xbuf[p], xpot[p], xlog[p])
        scores = lax.dot_general(
            left,
            ypack[...],
            (((0,), (0,)), ((), ())),
            preferred_element_type=jnp.float32,
        )
        peak = jnp.max(scores, 1, keepdims=True)
        mass = jnp.sum(jnp.exp2(scores - peak), 1, keepdims=True)
        tall = scores.reshape(rows // 8, 8, scores.shape[1])
        new = jnp.maximum(cmax[...], jnp.max(tall, 0))
        csum[...] = csum[...] * jnp.exp2(cmax[...] - new) + jnp.sum(
            jnp.exp2(tall - new[None]), 0
        )
        cmax[...] = new
        tile = jnp.where(
            lane == 0, peak, jnp.where(lane == 1, mass, jnp.where(lane == 2, tpeak, tmass))
        )
        msg = tile.T[:8]

        @pl.when(t > 0)
        def _():
            rowmsg[p] = msg
            rowcopy(me, p).start()

        @pl.when(t == 0)
        def _():
            rowres[me] = msg

        return 0

    lax.fori_loop(0, plane, step, 0)

    slog = jnp.concatenate([xlog[p] for p in range(plane)], 1)
    speak = jnp.max(slog)
    smass = jnp.sum(jnp.exp(slog - speak))
    peak = jnp.max(cmax[...], 0, keepdims=True)
    mass = jnp.sum(csum[...] * jnp.exp2(cmax[...] - peak), 0, keepdims=True)
    line = lax.broadcasted_iota(jnp.int32, (8, rows), 0)

    for q in range(outer):
        part = slice(q * rows, (q + 1) * rows)
        colmsg[q] = jnp.where(
            line == 0,
            peak[:, part],
            jnp.where(line == 1, mass[:, part], jnp.where(line == 2, speak, smass)),
        )
    for t in range(1, outer):
        colcopy(z, (z + t) % outer).start()
    colres[z] = colmsg[z]

    def combine(res, pot, logw):
        peaks = res[:, 0:1]
        top = jnp.max(peaks, 0)
        total = jnp.sum(res[:, 1:2] * jnp.exp2(peaks - top[None]), 0)
        lse = ln2 * (top + jnp.log2(total))
        wpeaks = res[:, 2:3]
        wtop = jnp.max(wpeaks, 0)
        wtotal = jnp.sum(res[:, 3:4] * jnp.exp(wpeaks - wtop[None]), 0)
        norm = wtop + jnp.log(wtotal)
        hat = -epsilon * (lse - logw - pot / epsilon - norm)
        return 0.5 * (pot + hat)

    for t in range(1, plane):
        p = (me + plane - t) % plane
        rowcopy(p, p).wait_recv()
    xout_ref[...] = combine(rowres[...], xpot[me], xlog[me])
    for t in range(1, outer):
        q = (z + outer - t) % outer
        colcopy(q, q).wait_recv()
    yout_ref[...] = combine(colres[...], ypot[z], ylog[z])

    for t in range(1, outer):
        q = (z + t) % outer
        for k in range(3):
            ycopy(k, z, q).wait_send()
        colcopy(z, q).wait_send()
    for t in range(1, plane):
        p = (me + t) % plane
        for k in range(3):
            xcopy(k, me, p).wait_send()
        rowcopy(me, p).wait_send()


def local(groups, members, x, y, xpot, ypot, xlog, ylog):
    inner = inner_size(groups, members)
    outer = members // inner
    plane = groups * inner
    feat, rows = x.shape
    span = outer * rows
    depth = 6 * feat + 16
    f32 = jnp.float32
    dma = pltpu.SemaphoreType.DMA
    out = pl.pallas_call(
        functools.partial(kernel, groups, inner, outer),
        out_shape=(jax.ShapeDtypeStruct((1, rows), f32),) * 2,
        in_specs=[pl.BlockSpec(memory_space=pl.ANY)] * 6,
        out_specs=(pl.BlockSpec(memory_space=pltpu.VMEM),) * 2,
        scratch_shapes=[
            pltpu.VMEM((plane, feat, rows), f32),
            pltpu.VMEM((plane, 1, rows), f32),
            pltpu.VMEM((plane, 1, rows), f32),
            pltpu.VMEM((outer, feat, rows), f32),
            pltpu.VMEM((outer, 1, rows), f32),
            pltpu.VMEM((outer, 1, rows), f32),
            pltpu.VMEM((depth, span), jnp.bfloat16),
            pltpu.VMEM((8, span), f32),
            pltpu.VMEM((8, span), f32),
            pltpu.VMEM((plane, 8, rows), f32),
            pltpu.VMEM((plane, 8, rows), f32),
            pltpu.VMEM((outer, 8, rows), f32),
            pltpu.VMEM((outer, 8, rows), f32),
            dma((6,)),
            dma((3, plane)),
            dma((3, plane)),
            dma((3, outer)),
            dma((3, outer)),
            dma((plane,)),
            dma((plane,)),
            dma((outer,)),
            dma((outer,)),
        ],
        compiler_params=pltpu.CompilerParams(collective_id=0, has_side_effects=True),
        name="sinkhorn",
    )(x, y, *(v.reshape(1, rows) for v in (xpot, ypot, xlog, ylog)))
    return tuple(v.reshape(rows) for v in out)


def solution(mesh):
    both = ("grp", "mem")
    return jax.shard_map(
        functools.partial(local, mesh.shape["grp"], mesh.shape["mem"]),
        mesh=mesh,
        in_specs=(P(None, both), P(None, both), P(both), P(both), P(both), P(both)),
        out_specs=(P(both), P(both)),
        check_vma=False,
    )
```

```python
import functools
import math

import jax
import jax.numpy as jnp
from jax import lax
from jax.experimental import pallas as pl
from jax.experimental.pallas import tpu as pltpu
from jax.sharding import PartitionSpec as P

MESH = pl.DeviceIdType.MESH
epsilon = 4.0
log2e = math.log2(math.e)
ln2 = math.log(2.0)


def inner_size(groups, members):
    inner = 1
    while members % inner or groups * inner < members // inner:
        inner += 1
    return inner


def split3(v):
    hi = v.astype(jnp.bfloat16)
    rest = v - hi.astype(jnp.float32)
    mid = rest.astype(jnp.bfloat16)
    low = (rest - mid.astype(jnp.float32)).astype(jnp.bfloat16)
    return hi, mid, low


def term_of(points, pot, logw):
    half = 0.5 * jnp.sum(points * points, 0, keepdims=True)
    return (logw + (pot - half) / epsilon) * log2e


def extra_rows(term, first):
    width = term.shape[1]
    hi, mid, low = (v.astype(jnp.float32) for v in split3(term))
    line = lax.broadcasted_iota(jnp.int32, (16, width), 0)
    base = 0 if first else 3
    ones = 3 - base
    out = jnp.where((line >= ones) & (line < ones + 3), 1.0, 0.0)
    for k, part in enumerate((hi, mid, low)):
        out = jnp.where(line == base + k, part, out)
    return out.astype(jnp.bfloat16)


def pack_left(points, pot, logw):
    hi, mid, low = split3(points * (log2e / epsilon))
    return jnp.concatenate(
        [hi, hi, mid, mid, hi, low, extra_rows(term_of(points, pot, logw), True)], 0
    )


def pack_right(points, pot, logw):
    hi, mid, low = split3(points)
    return jnp.concatenate(
        [hi, mid, hi, mid, low, hi, extra_rows(term_of(points, pot, logw), False)], 0
    )


def kernel(
    groups,
    inner,
    outer,
    x_ref,
    y_ref,
    xpot_ref,
    ypot_ref,
    xlog_ref,
    ylog_ref,
    xout_ref,
    yout_ref,
    xbuf,
    xpot,
    xlog,
    ybuf,
    ypot,
    ylog,
    ypack,
    lpack,
    cmax,
    csum,
    rowmsg,
    rowres,
    colmsg,
    colres,
    local_sem,
    xsend,
    xrecv,
    ysend,
    yrecv,
    rsend,
    rrecv,
    csend,
    crecv,
):
    chunks = 2 - outer % 2
    half = outer // chunks
    plane = groups * inner
    rows = xbuf.shape[2]
    g = lax.axis_index("grp")
    mem = lax.axis_index("mem")
    z = mem // inner
    i = mem % inner
    me = g * inner + i

    def plane_dev(p):
        return (p // inner, z * inner + p % inner)

    def outer_dev(q):
        return (g, q * inner + i)

    xs = ((x_ref, xbuf), (xpot_ref, xpot), (xlog_ref, xlog))
    ys = ((y_ref, ybuf), (ypot_ref, ypot), (ylog_ref, ylog))
    locals_ = [
        pltpu.make_async_copy(src, dst.at[slot], local_sem.at[k])
        for k, (src, dst, slot) in enumerate(
            [(s, d, z) for s, d in ys] + [(s, d, me) for s, d in xs]
        )
    ]
    for c in locals_:
        c.start()

    barrier = pltpu.get_barrier_semaphore()
    for t in range(1, plane):
        pl.semaphore_signal(
            barrier, inc=1, device_id=plane_dev((me + t) % plane), device_id_type=MESH
        )
    for t in range(1, outer):
        pl.semaphore_signal(
            barrier, inc=1, device_id=outer_dev((z + t) % outer), device_id_type=MESH
        )
    for c in locals_:
        c.wait()
    pl.semaphore_wait(barrier, plane + outer - 2)

    def xcopy(k, slot, dest):
        dst = xs[k][1]
        return pltpu.make_async_remote_copy(
            src_ref=dst.at[slot],
            dst_ref=dst.at[slot],
            send_sem=xsend.at[k, dest],
            recv_sem=xrecv.at[k, slot],
            device_id=plane_dev(dest),
            device_id_type=MESH,
        )

    def ycopy(k, slot, dest):
        dst = ys[k][1]
        return pltpu.make_async_remote_copy(
            src_ref=dst.at[slot],
            dst_ref=dst.at[slot],
            send_sem=ysend.at[k, dest],
            recv_sem=yrecv.at[k, slot],
            device_id=outer_dev(dest),
            device_id_type=MESH,
        )

    def rowcopy(chunk, slot, dest):
        return pltpu.make_async_remote_copy(
            src_ref=rowmsg.at[chunk * plane + dest],
            dst_ref=rowres.at[chunk * plane + slot],
            send_sem=rsend.at[chunk * plane + dest],
            recv_sem=rrecv.at[chunk * plane + slot],
            device_id=plane_dev(dest),
            device_id_type=MESH,
        )

    def colcopy(slot, dest):
        return pltpu.make_async_remote_copy(
            src_ref=colmsg.at[dest],
            dst_ref=colres.at[slot],
            send_sem=csend.at[dest],
            recv_sem=crecv.at[slot],
            device_id=outer_dev(dest),
            device_id_type=MESH,
        )

    def block_of(chunk, t):
        return (z // half + chunk) % chunks * half + (z + t) % half

    for chunk in range(chunks):
        for t in range(chunk == 0, half):
            for k in range(3):
                ycopy(k, z, block_of(chunk, t)).start()
    for t in range(1, plane):
        for k in range(3):
            xcopy(k, me, (me + plane - t) % plane).start()

    cmax[...] = jnp.full(cmax.shape, -3e38, jnp.float32)
    csum[...] = jnp.zeros(csum.shape, jnp.float32)
    lane = lax.broadcasted_iota(jnp.int32, (rows, 128), 1)

    for chunk in range(chunks):
        logs = []
        for t in range(half):
            q = block_of(chunk, t)
            if chunk or t:
                for k in range(3):
                    ycopy(k, q, q).wait_recv()
            at = pl.ds(pl.multiple_of(q * rows, rows), rows)
            ypack[:, at] = pack_right(ybuf[q], ypot[q], ylog[q])
            logs.append(ylog[q])
        tlog = jnp.concatenate(logs, 1)
        tpeak = jnp.max(tlog)
        tmass = jnp.sum(jnp.exp(tlog - tpeak))
        width = half * rows
        begin = (z // half + chunk) % chunks * width
        cols = pl.ds(pl.multiple_of(begin, rows), width)

        def step(t, _, chunk=chunk, tpeak=tpeak, tmass=tmass, cols=cols):
            p = (me + t) % plane

            if chunk == 0:

                @pl.when(t > 0)
                def _():
                    for k in range(3):
                        xcopy(k, p, p).wait_recv()

                left = pack_left(xbuf[p], xpot[p], xlog[p])
                lpack[p] = left
            else:
                left = lpack[p]
            scores = lax.dot_general(
                left,
                ypack[:, cols],
                (((0,), (0,)), ((), ())),
                preferred_element_type=jnp.float32,
            )
            peak = jnp.max(scores, 1, keepdims=True)
            mass = jnp.sum(jnp.exp2(scores - peak), 1, keepdims=True)
            tall = scores.reshape(rows // 8, 8, scores.shape[1])
            old = cmax[:, cols]
            new = jnp.maximum(old, jnp.max(tall, 0))
            csum[:, cols] = csum[:, cols] * jnp.exp2(old - new) + jnp.sum(
                jnp.exp2(tall - new[None]), 0
            )
            cmax[:, cols] = new
            tile = jnp.where(
                lane == 0,
                peak,
                jnp.where(lane == 1, mass, jnp.where(lane == 2, tpeak, tmass)),
            )
            msg = tile.T[:8]

            @pl.when(t > 0)
            def _():
                rowmsg[chunk * plane + p] = msg
                rowcopy(chunk, me, p).start()

            @pl.when(t == 0)
            def _():
                rowres[chunk * plane + me] = msg

            return 0

        lax.fori_loop(0, plane, step, 0)

    slog = jnp.concatenate([xlog[p] for p in range(plane)], 1)
    speak = jnp.max(slog)
    smass = jnp.sum(jnp.exp(slog - speak))
    peak = jnp.max(cmax[...], 0, keepdims=True)
    mass = jnp.sum(csum[...] * jnp.exp2(cmax[...] - peak), 0, keepdims=True)
    line = lax.broadcasted_iota(jnp.int32, (8, rows), 0)

    for q in range(outer):
        part = slice(q * rows, (q + 1) * rows)
        colmsg[q] = jnp.where(
            line == 0,
            peak[:, part],
            jnp.where(line == 1, mass[:, part], jnp.where(line == 2, speak, smass)),
        )
    for t in range(1, outer):
        colcopy(z, (z + t) % outer).start()
    colres[z] = colmsg[z]

    def combine(res, pot, logw):
        peaks = res[:, 0:1]
        top = jnp.max(peaks, 0)
        total = jnp.sum(res[:, 1:2] * jnp.exp2(peaks - top[None]), 0)
        lse = ln2 * (top + jnp.log2(total))
        wpeaks = res[:, 2:3]
        wtop = jnp.max(wpeaks, 0)
        wtotal = jnp.sum(res[:, 3:4] * jnp.exp(wpeaks - wtop[None]), 0)
        norm = wtop + jnp.log(wtotal)
        return -epsilon * (lse - logw - pot / epsilon - norm)

    for t in range(1, plane):
        p = (me + plane - t) % plane
        for chunk in range(chunks):
            rowcopy(chunk, p, p).wait_recv()
    xout_ref[...] = combine(rowres[...], xpot[me], xlog[me])
    for t in range(1, outer):
        q = (z + outer - t) % outer
        colcopy(q, q).wait_recv()
    yout_ref[...] = combine(colres[...], ypot[z], ylog[z])

    for t in range(1, outer):
        q = (z + t) % outer
        for k in range(3):
            ycopy(k, z, q).wait_send()
        colcopy(z, q).wait_send()
    for t in range(1, plane):
        p = (me + t) % plane
        for k in range(3):
            xcopy(k, me, p).wait_send()
        for chunk in range(chunks):
            rowcopy(chunk, me, p).wait_send()


def local(groups, members, x, y, xpot, ypot, xlog, ylog):
    inner = inner_size(groups, members)
    outer = members // inner
    chunks = 2 - outer % 2
    plane = groups * inner
    feat, rows = x.shape
    span = outer * rows
    depth = 6 * feat + 16
    f32 = jnp.float32
    dma = pltpu.SemaphoreType.DMA
    out = pl.pallas_call(
        functools.partial(kernel, groups, inner, outer),
        out_shape=(jax.ShapeDtypeStruct((1, rows), f32),) * 2,
        in_specs=[pl.BlockSpec(memory_space=pl.ANY)] * 6,
        out_specs=(pl.BlockSpec(memory_space=pltpu.VMEM),) * 2,
        scratch_shapes=[
            pltpu.VMEM((plane, feat, rows), f32),
            pltpu.VMEM((plane, 1, rows), f32),
            pltpu.VMEM((plane, 1, rows), f32),
            pltpu.VMEM((outer, feat, rows), f32),
            pltpu.VMEM((outer, 1, rows), f32),
            pltpu.VMEM((outer, 1, rows), f32),
            pltpu.VMEM((depth, span), jnp.bfloat16),
            pltpu.VMEM((plane, depth, rows), jnp.bfloat16),
            pltpu.VMEM((8, span), f32),
            pltpu.VMEM((8, span), f32),
            pltpu.VMEM((chunks * plane, 8, rows), f32),
            pltpu.VMEM((chunks * plane, 8, rows), f32),
            pltpu.VMEM((outer, 8, rows), f32),
            pltpu.VMEM((outer, 8, rows), f32),
            dma((6,)),
            dma((3, plane)),
            dma((3, plane)),
            dma((3, outer)),
            dma((3, outer)),
            dma((chunks * plane,)),
            dma((chunks * plane,)),
            dma((outer,)),
            dma((outer,)),
        ],
        compiler_params=pltpu.CompilerParams(collective_id=0, has_side_effects=True),
        name="sinkhorn",
    )(x, y, *(v.reshape(1, rows) for v in (xpot, ypot, xlog, ylog)))
    return tuple(0.5 * (pot + v.reshape(rows)) for v, pot in zip(out, (xpot, ypot)))


def solution(mesh):
    both = ("grp", "mem")
    return jax.shard_map(
        functools.partial(local, mesh.shape["grp"], mesh.shape["mem"]),
        mesh=mesh,
        in_specs=(P(None, both), P(None, both), P(both), P(both), P(both), P(both)),
        out_specs=(P(both), P(both)),
        check_vma=False,
    )
```
